32 devices in a mesh: clip: 2 (over y), ha: 4 (over z), wa: 4 (over x, core).
Axes of the slice: x: 2, y: 2, z: 4, core: 2. Of those that a mesh axis runs over, the one named last changes fastest.
Arguments:
- cotangent: float32 [8, 16, 256, 96], P('clip', 'ha', 'wa'), parts along dimension 0, may hold values from -6 to 6
- stored_first: float32 [8, 16, 256, 96], P('clip', 'ha', 'wa'), parts along dimension 0, may hold values from -8 to 8
- stored_second: float32 [8, 16, 256, 96], P('clip', 'ha', 'wa'), parts along dimension 0, may hold values from -8 to 8
- w_first: float32 [3, 3, 3, 96, 96], replicated, may hold values from -0.125 to 0.125
- w_second: float32 [3, 3, 3, 96, 96], replicated, may hold values from -0.125 to 0.125
- w_third: float32 [3, 3, 3, 96, 96], replicated, may hold values from -0.125 to 0.125
Outputs:
- input_grad: float32 [8, 16, 256, 96], P('clip', 'ha', 'wa'), parts along dimension 0
The draws below stay inside these ranges and needn't reach their ends.
There are 2 independent parts, one for each index of `clip`. The reference program is written for one: setup_inputs(seed, part) draws one part's arguments, and reference() takes and returns one part's arrays. A program takes and returns all parts, laid end to end along the dimension named above; an argument that names none is the same for every part. Nothing has to cross between parts.
All inputs are finite; a program needn't handle non-finite values.
Results may differ from the reference program's by a relative error of at most 0.00013.
Values sent between devices are 32-bit elements; how exact they have to be, the bound alone decides.
A program may use at most 64 MiB of HBM per device.

```python
import jax
import jax.numpy as jnp
from jax import lax

C = 96
F = 4
H = 16
W = 256


def levels(stream_key, extent, shards, smallest, top_value):
    loudness, own = 1.0, jax.random.fold_in(stream_key, 6)
    for position, parts in shards:
        steps = jnp.exp(jax.random.uniform(jax.random.fold_in(own, position), (parts,), jnp.float32, smallest / len(shards), top_value / len(shards)))
        loudness = loudness * jnp.repeat(steps, extent[position] // parts).reshape([-1 if axis == position else 1 for axis in range(len(extent))])
    return loudness


def bell_draw(key, dims, scale, limit, cuts=(), kind=jnp.bfloat16):
    drawn = scale * jax.random.normal(key, dims, jnp.float32)
    if cuts:
        drawn = drawn * levels(key, dims, cuts, -0.22, 0.18)
    return jnp.clip(drawn, -limit, limit).astype(kind)


def setup_inputs(seed: int = 0, part: int = 0) -> dict:
    splits = jax.random.split(jax.random.key(seed), 7)
    own_keys = jax.random.split(jax.random.fold_in(splits[6], part), 7)
    cotangent = bell_draw(own_keys[0], (F, H, W, C), 1.0, 6.0, ((1, 4), (2, 4)), jnp.float32)
    stored_first = bell_draw(own_keys[1], (F, H, W, C), 2.0, 8.0, ((1, 4), (2, 4)), jnp.float32)
    stored_second = bell_draw(own_keys[2], (F, H, W, C), 2.0, 8.0, ((1, 4), (2, 4)), jnp.float32)
    w_first = bell_draw(splits[3], (3, 3, 3, C, C), (27 * C) ** -0.5, 0.125, (), jnp.float32)
    w_second = bell_draw(splits[4], (3, 3, 3, C, C), (27 * C) ** -0.5, 0.125, (), jnp.float32)
    w_third = bell_draw(splits[5], (3, 3, 3, C, C), (27 * C) ** -0.5, 0.125, (), jnp.float32)
    return dict(cotangent=cotangent, stored_first=stored_first, stored_second=stored_second, w_first=w_first, w_second=w_second, w_third=w_third)


def back_conv(gradient, kernel):
    padded = jnp.pad(gradient, ((0, 2), (1, 1), (1, 1), (0, 0)))
    flipped = jnp.transpose(jnp.flip(kernel, (0, 1, 2)), (0, 1, 2, 4, 3))
    result = lax.conv_general_dilated(padded[None], flipped, (1, 1, 1), "VALID",
                                      dimension_numbers=("NDHWC", "DHWIO", "NDHWC"),
                                      precision=lax.Precision.HIGHEST)
    return result[0]


def silu_slope(value):
    sigma = jax.nn.sigmoid(value)
    return sigma * (1.0 + value * (1.0 - sigma))


def reference(cotangent, stored_first, stored_second, w_first, w_second, w_third):
    second_grad = back_conv(cotangent, w_third) * silu_slope(stored_second)
    first_grad = back_conv(second_grad, w_second) * silu_slope(stored_first)
    return back_conv(first_grad, w_first)
```

```python
import functools

import jax
import jax.numpy as jnp
from jax import lax
from jax.experimental import pallas as pl
from jax.experimental.pallas import tpu as pltpu
from jax.sharding import PartitionSpec as P

LANES = 128
EDGE = 8
SIDES = tuple((dh, dw) for dh in (-1, 0, 1) for dw in (-1, 0, 1) if (dh, dw) != (0, 0))
COLS = ((0, -1), (0, 1))
ROWS = tuple(s for s in SIDES if s[0] != 0)


def silu_slope(value):
    sigma = 1.0 / (1.0 + jnp.exp(-value))
    return sigma * (1.0 + value * (1.0 - sigma))


def split(value):
    high = value.astype(jnp.bfloat16)
    low = (value - high.astype(jnp.float32)).astype(jnp.bfloat16)
    return high, low


def kernel(
    sizes, cot, first, second, w1, w2, w3, out,
    ext0, ext1, ext2, xs, wbuf0, wbuf1, wbuf2, whl, acc, sfirst, ssecond,
    local_sem, send_sem, recv_sem,
):
    nh, nw, F, R, W, C = sizes
    span = 3 * LANES
    exts = (ext0, ext1, ext2)
    wbufs = (wbuf0, wbuf1, wbuf2)
    ih, iw = lax.axis_index("ha"), lax.axis_index("wa")

    def present(dh, dw):
        ok = ih >= 0
        if dh:
            ok = ok & ((ih > 0) if dh < 0 else (ih < nh - 1))
        if dw:
            ok = ok & ((iw > 0) if dw < 0 else (iw < nw - 1))
        return ok

    def one(flag):
        return jnp.where(flag, jnp.int32(1), jnp.int32(0))

    loads = [
        pltpu.make_async_copy(cot, ext0.at[:, pl.ds(1, R), pl.ds(EDGE, W), :], local_sem.at[0]),
        pltpu.make_async_copy(w3, wbuf0, local_sem.at[1]),
        pltpu.make_async_copy(w2, wbuf1, local_sem.at[2]),
        pltpu.make_async_copy(w1, wbuf2, local_sem.at[3]),
        pltpu.make_async_copy(second, ssecond, local_sem.at[4]),
        pltpu.make_async_copy(first, sfirst, local_sem.at[5]),
    ]
    for load in loads:
        load.start()

    barrier = pltpu.get_barrier_semaphore()
    for dh, dw in SIDES:
        @pl.when(present(dh, dw))
        def _():
            pl.semaphore_signal(
                barrier, inc=1, device_id={"ha": ih + dh, "wa": iw + dw},
                device_id_type=pl.DeviceIdType.MESH,
            )
    tall = 1 + one(ih > 0) + one(ih < nh - 1)
    wide = 1 + one(iw > 0) + one(iw < nw - 1)
    pl.semaphore_wait(barrier, tall * wide - 1)

    groups = ((F // 2, F), (0, F // 2))

    def copy_to(phase, group, dh, dw):
        t0, t1 = groups[group]
        row, rows = {-1: (0, 1), 0: (0, R), 1: (R - 1, 1)}[dh]
        col, cols = {-1: (0, EDGE), 0: (0, W), 1: (W - EDGE, EDGE)}[dw]
        drow = {-1: R + 1, 0: 1, 1: 0}[dh]
        dcol = {-1: EDGE + W, 0: EDGE, 1: 0}[dw]
        ext, frames = exts[phase], pl.ds(t0, t1 - t0)
        if phase == 0:
            src = cot.at[frames, pl.ds(row, rows), pl.ds(col, cols), :]
        else:
            src = ext.at[frames, pl.ds(row + 1, rows), pl.ds(col + EDGE, cols), :]
        at = SIDES.index((dh, dw))
        return pltpu.make_async_remote_copy(
            src_ref=src,
            dst_ref=ext.at[frames, pl.ds(drow, rows), pl.ds(dcol, cols), :],
            send_sem=send_sem.at[phase, group, at],
            recv_sem=recv_sem.at[phase, group, at],
            device_id={"ha": ih + dh, "wa": iw + dw},
            device_id_type=pl.DeviceIdType.MESH,
        )

    def send(phase, group):
        for dh, dw in COLS + ROWS:
            @pl.when(present(dh, dw))
            def _():
                copy_to(phase, group, dh, dw).start()

    def receive(phase, group, sides):
        for dh, dw in sides:
            @pl.when(present(-dh, -dw))
            def _():
                copy_to(phase, group, dh, dw).wait_recv()

    send(0, 0)
    send(0, 1)

    xs[...] = jnp.zeros_like(xs)
    for dh, dw in SIDES:
        @pl.when(jnp.logical_not(present(dh, dw)))
        def _():
            row, rows = {-1: (0, 1), 0: (1, R), 1: (R + 1, 1)}[dh]
            col, cols = {-1: (0, EDGE), 0: (EDGE, W), 1: (EDGE + W, EDGE)}[dw]
            for ext in exts:
                ext[:, row : row + rows, col : col + cols, :] = jnp.zeros(
                    (F, rows, cols, C), jnp.float32
                )

    def prepare(phase):
        wbuf = wbufs[phase]

        @pl.loop(0, 3)
        def _(i):
            for j in range(3):
                for k in range(3):
                    turned = split(jnp.transpose(wbuf[i, j, k]))
                    for part in range(2):
                        at = part * span + k * LANES
                        whl[phase, i, j, at : at + C, 0:C] = turned[part]
                        whl[phase, i, j, at + C : at + LANES, :] = jnp.zeros(
                            (LANES - C, LANES), jnp.bfloat16
                        )

    def arrange(phase, group, rows):
        ext = exts[phase]

        @pl.loop(*groups[group])
        def _(f):
            for e in rows:
                for k in range(3):
                    start = EDGE + 1 - k
                    high, low = split(ext[f, e, start : start + W, :])
                    xs[f, e, :, k * LANES : k * LANES + C] = high
                    xs[f, e, :, span + k * LANES : span + k * LANES + C] = low

    pairs = R // 2

    def reach(group, i):
        t0, t1 = groups[group]
        return t0, min(t1, F - 2 + i)

    def lhs(group, i, q):
        t0, t1 = reach(group, i)
        parts = [xs[t0 + 2 - i : t1 + 2 - i, 2 * p + q][:, None] for p in range(pairs)]
        block = jnp.concatenate(parts, axis=1).reshape((t1 - t0) * pairs * W, 2 * span)
        return jnp.concatenate([block, block[:, :span]], axis=1)

    def rhs(phase, i, j):
        high, low = whl[phase, i, j, :span], whl[phase, i, j, span:]
        return jnp.concatenate([high, high, low], axis=0)

    def dot(a, b):
        return jnp.dot(a, b, preferred_element_type=jnp.float32)

    def weights(phase, i, j):
        if 0 <= j <= 2:
            return rhs(phase, i, j)
        return jnp.zeros((3 * span, LANES), jnp.bfloat16)

    def multiply(phase, group, offsets, fresh):
        for i in (2, 1, 0):
            t0, t1 = reach(group, i)
            if t1 <= t0:
                continue
            a = jnp.concatenate([lhs(group, i, q) for q in offsets], axis=1)
            b = jnp.concatenate(
                [
                    jnp.concatenate([weights(phase, i, 2 - q), weights(phase, i, 3 - q)], axis=1)
                    for q in offsets
                ],
                axis=0,
            )
            value = dot(a, b).reshape(t1 - t0, pairs, W, 2 * LANES)
            if fresh and i == 2:
                acc[t0:t1] = value
            else:
                acc[t0:t1] += value

    for phase in range(3):
        loads[phase + 1].wait()
        prepare(phase)
    loads[0].wait()
    for phase in range(3):
        for group in range(2):
            t0, t1 = groups[group]
            if phase and group == 0:
                receive(phase, group, SIDES)
                arrange(phase, group, range(R + 2))
                multiply(phase, group, (0, 1, 2, 3), True)
            else:
                receive(phase, group, COLS)
                arrange(phase, group, range(1, R + 1))
                multiply(phase, group, (1, 2), True)
                receive(phase, group, ROWS)
                arrange(phase, group, (0, R + 1))
                multiply(phase, group, (0, 3), False)
            if phase < 2 and group == 0:
                loads[4 + phase].wait()
            for h in range(R):
                at = h % 2 * LANES
                value = acc[t0:t1, h // 2, :, at : at + C]
                if phase < 2:
                    stored = (ssecond, sfirst)[phase]
                    exts[phase + 1][t0:t1, h + 1, EDGE : EDGE + W, :] = value * silu_slope(
                        stored[t0:t1, h]
                    )
                else:
                    out[t0:t1, h] = value
            if phase < 2:
                send(phase + 1, group)

    for phase in range(3):
        for group in range(2):
            for dh, dw in SIDES:
                @pl.when(present(dh, dw))
                def _():
                    copy_to(phase, group, dh, dw).wait_send()


def local(cotangent, stored_first, stored_second, w_first, w_second, w_third):
    F, R, W, C = cotangent.shape
    sizes = (lax.axis_size("ha"), lax.axis_size("wa"), F, R, W, C)
    ext = pltpu.VMEM((F, R + 2, W + 2 * EDGE, C), jnp.float32)
    wbuf = pltpu.VMEM(w_first.shape, jnp.float32)
    stored = pltpu.VMEM((F, R, W, C), jnp.float32)
    return pl.pallas_call(
        functools.partial(kernel, sizes),
        out_shape=pltpu.VMEM(cotangent.shape, jnp.float32),
        in_specs=[pl.BlockSpec(memory_space=pltpu.HBM)] * 6,
        out_specs=pl.BlockSpec(memory_space=pltpu.VMEM),
        scratch_shapes=[
            ext, ext, ext,
            pltpu.VMEM((F, R + 2, W, 6 * LANES), jnp.bfloat16),
            wbuf, wbuf, wbuf,
            pltpu.VMEM((3, 3, 3, 6 * LANES, LANES), jnp.bfloat16),
            pltpu.VMEM((F, R // 2, W, 2 * LANES), jnp.float32),
            stored, stored,
            pltpu.SemaphoreType.DMA((6,)),
            pltpu.SemaphoreType.DMA((3, 2, 8)),
            pltpu.SemaphoreType.DMA((3, 2, 8)),
        ],
        compiler_params=pltpu.CompilerParams(
            collective_id=0, has_side_effects=True, vmem_limit_bytes=67043328 - cotangent.size * 6
        ),
    )(cotangent, stored_first, stored_second, w_first, w_second, w_third)


def solution(mesh):
    split_spec = P("clip", "ha", "wa", None)
    return jax.shard_map(
        local,
        mesh=mesh,
        in_specs=(split_spec, split_spec, split_spec, P(), P(), P()),
        out_specs=split_spec,
        check_vma=False,
    )
```

```python
import functools

import jax
import jax.numpy as jnp
from jax import lax
from jax.experimental import pallas as pl
from jax.experimental.pallas import tpu as pltpu
from jax.sharding import PartitionSpec as P

LANES = 128
NB = 4
SIDES = tuple((dh, dw) for dh in (-1, 0, 1) for dw in (-1, 0, 1) if (dh, dw) != (0, 0))
CORNERS = tuple(s for s in SIDES if s[0] and s[1])
COLS = ((0, -1), (0, 1))
ROWS = ((-1, 0), (1, 0))
ORDER = CORNERS + COLS + ROWS


def silu_slope(value):
    sigma = 1.0 / (1.0 + jnp.exp(-value))
    return sigma * (1.0 + value * (1.0 - sigma))


def split(value):
    high = value.astype(jnp.bfloat16)
    low = (value - high.astype(jnp.float32)).astype(jnp.bfloat16)
    return high, low


def kernel(
    sizes, cot, first, second, w1, w2, w3, out,
    vcot, sfirst, ssecond, slopes, wbuf0, wbuf1, wbuf2, wh, own, lhs, acc,
    zsend, zrecv, xsend, xrecv, crecv,
    local_sem, send_sem, recv_sem,
):
    nh, nw, F, R, W, C = sizes
    A, pairs = W // NB, R // 2
    rows = NB * pairs * A
    wbufs = (wbuf0, wbuf1, wbuf2)
    ih, iw = lax.axis_index("ha"), lax.axis_index("wa")

    def present(dh, dw):
        ok = ih >= 0
        if dh:
            ok = ok & ((ih > 0) if dh < 0 else (ih < nh - 1))
        if dw:
            ok = ok & ((iw > 0) if dw < 0 else (iw < nw - 1))
        return ok

    def one(flag):
        return jnp.where(flag, jnp.int32(1), jnp.int32(0))

    barrier = pltpu.get_barrier_semaphore()
    for dh, dw in SIDES:
        @pl.when(present(dh, dw))
        def _():
            pl.semaphore_signal(
                barrier, inc=1, device_id={"ha": ih + dh, "wa": iw + dw},
                device_id_type=pl.DeviceIdType.MESH,
            )

    loads = [
        pltpu.make_async_copy(cot, vcot, local_sem.at[0]),
        pltpu.make_async_copy(w3, wbuf0, local_sem.at[1]),
        pltpu.make_async_copy(second, ssecond, local_sem.at[4]),
        pltpu.make_async_copy(w2, wbuf1, local_sem.at[2]),
        pltpu.make_async_copy(first, sfirst, local_sem.at[5]),
        pltpu.make_async_copy(w1, wbuf2, local_sem.at[3]),
    ]
    for load in loads:
        load.start()

    def side(d):
        return (d + 1) // 2

    def landing(phase, t, dh, dw):
        if dh and dw:
            return crecv.at[phase, t, side(dh), side(dw)]
        if dw:
            return xrecv.at[phase, t, side(dw)]
        return zrecv.at[phase, t, side(dh)]

    def copy_to(phase, t, dh, dw):
        at = SIDES.index((dh, dw))
        source = xsend.at[phase, t, side(dw)] if dw else zsend.at[phase, t, side(dh)]
        return pltpu.make_async_remote_copy(
            src_ref=source,
            dst_ref=landing(phase, t, -dh, -dw),
            send_sem=send_sem.at[phase, t, at],
            recv_sem=recv_sem.at[phase, t, at],
            device_id={"ha": ih + dh, "wa": iw + dw},
            device_id_type=pl.DeviceIdType.MESH,
        )

    def send(phase, t):
        for dh, dw in ORDER:
            @pl.when(present(dh, dw))
            def _():
                copy_to(phase, t, dh, dw).start()

    def receive(phase, t):
        for dh, dw in ORDER:
            @pl.when(present(-dh, -dw))
            def _():
                copy_to(phase, t, dh, dw).wait_recv()

    for dh, dw in SIDES:
        @pl.when(jnp.logical_not(present(dh, dw)))
        def _():
            for phase in range(3):
                for t in range(F):
                    ref = landing(phase, t, dh, dw)
                    ref[...] = jnp.zeros(ref.shape, jnp.float32)

    lane = lax.broadcasted_iota(jnp.int32, (A, LANES), 1)
    line = lax.broadcasted_iota(jnp.int32, (A, LANES), 0)
    real = lane < C
    third = C // 3

    def wide(value):
        return jnp.concatenate(
            [value, jnp.zeros((value.shape[0], LANES - C), jnp.float32)], axis=1
        )

    def place(b, r):
        return (b * pairs + r // 2) * A

    def post(phase, t, tile):
        for r, to in ((0, 0), (R - 1, 1)):
            last = tile(r, NB - 1)
            for m in range(3):
                moved = pltpu.roll(last, LANES - third - third * m, axis=1)
                zsend[phase, t, to, m * A : (m + 1) * A, :] = jnp.where(real, tile(r, m), moved)
        for r in range(R):
            xsend[phase, t, 0, r : r + 1, :] = tile(r, 0)[0:1]
            xsend[phase, t, 1, r : r + 1, :] = tile(r, NB - 1)[A - 1 : A]

    def unpack(phase, t, to):
        packed = [zrecv[phase, t, to, m * A : (m + 1) * A, :] for m in range(3)]
        moved = [pltpu.roll(packed[m], third + third * m, axis=1) for m in range(3)]
        last = jnp.where(lane < third, moved[0], jnp.where(lane < 2 * third, moved[1], moved[2]))
        return [jnp.where(real, v, 0.0) for v in packed + [last]]

    xsend[...] = jnp.zeros_like(xsend)
    loads[0].wait()

    for t in reversed(range(F)):
        tiles = {}
        for r in range(R):
            for b in range(NB):
                tiles[r, b] = wide(vcot[t, r, pl.ds(b, A, stride=NB), :])
                own[0, t, r % 2, place(b, r) : place(b, r) + A, :] = tiles[r, b]
        post(0, t, lambda r, b: tiles[r, b])

    tall = 1 + one(ih > 0) + one(ih < nh - 1)
    broad = 1 + one(iw > 0) + one(iw < nw - 1)
    pl.semaphore_wait(barrier, tall * broad - 1)
    for t in reversed(range(F)):
        send(0, t)

    def prepare(phase):
        wbuf = wbufs[phase]

        @pl.loop(0, 3)
        def _(i):
            for k in range(3):
                g0, g1, g2 = (wide(wbuf[i, 2 - e, k]) for e in range(3))
                even, odd = (g0 + g2) * 0.5, g1 * 0.5
                for q, value in enumerate((g0, even + odd, even - odd, g2)):
                    high, low = split(value)
                    at = k * LANES
                    wh[phase, i, q, 0:C, at : at + LANES] = high
                    wh[phase, i, q, LANES : LANES + C, at : at + LANES] = low

    def slope_of(stored, at):
        @pl.loop(0, F)
        def _(t):
            for r in range(R):
                for b in range(NB):
                    slopes[at, t, r % 2, place(b, r) : place(b, r) + A, :] = wide(
                        silu_slope(stored[t, r, pl.ds(b, A, stride=NB), :])
                    )

    loads[1].wait()
    prepare(0)
    loads[2].wait()
    slope_of(ssecond, 0)
    loads[3].wait()
    prepare(1)
    loads[4].wait()
    slope_of(sfirst, 1)
    loads[5].wait()
    prepare(2)

    def arrange(phase, t):
        tiles = {}
        for r in range(-1, R + 1):
            if 0 <= r < R:
                for b in range(NB):
                    tiles[r, b] = own[phase, t, r % 2, place(b, r) : place(b, r) + A, :]
                left, right = (xrecv[phase, t, s, r : r + 1, :] for s in range(2))
            else:
                to = 0 if r < 0 else 1
                for b, value in enumerate(unpack(phase, t, to)):
                    tiles[r, b] = value
                near = R - 1 if r < 0 else 0
                left, right = (crecv[phase, t, to, s, near : near + 1, :] for s in range(2))
            tiles[r, -1] = jnp.where(line == 0, left, pltpu.roll(tiles[r, NB - 1], 1, axis=0))
            tiles[r, NB] = jnp.where(line == A - 1, right, pltpu.roll(tiles[r, 0], A - 1, axis=0))
        for p in range(pairs):
            for b in range(-1, NB + 1):
                d0, d1, d2, d3 = (tiles[2 * p - 1 + n, b] for n in range(4))
                for q, value in enumerate((d0 - d2, d1 + d2, d2 - d1, d1 - d3)):
                    high, low = split(value)
                    lhs[t, q, b + 1, p * A : (p + 1) * A, 0:LANES] = high
                    lhs[t, q, b + 1, p * A : (p + 1) * A, LANES:] = low

    def product(phase, t, i, q):
        a = jnp.concatenate(
            [lhs[t, q, 2 - k : 2 - k + NB].reshape(rows, 2 * LANES) for k in range(3)], axis=1
        )
        w = [wh[phase, i, q, :, k * LANES : (k + 1) * LANES] for k in range(3)]
        b = jnp.concatenate([w[0], w[0], w[1], w[1], w[2], w[2]], axis=1)
        value = lax.dot_general(
            a, b, (((1,), (1,)), ((), ())), preferred_element_type=jnp.float32
        )
        return value[:, :LANES] + value[:, LANES:]

    allreal = lax.broadcasted_iota(jnp.int32, (rows, LANES), 1) < C

    for phase in range(3):
        for t in reversed(range(F)):
            receive(phase, t)
            arrange(phase, t)
            m = []
            for q in range(4):
                value = product(phase, t, 2, q)
                m.append(value if t == F - 1 else value + acc[t, q])
            done = (m[0] + m[1] + m[2], m[1] - m[2] - m[3])
            if phase < 2:
                done = [jnp.where(allreal, done[s] * slopes[phase, t, s], 0.0) for s in range(2)]
                for s in range(2):
                    own[phase + 1, t, s] = done[s]
                post(phase + 1, t, lambda r, b: done[r % 2][place(b, r) : place(b, r) + A])
                send(phase + 1, t)
            else:
                for r in range(R):
                    for b in range(NB):
                        out[t, r, pl.ds(b, A, stride=NB), :] = done[r % 2][
                            place(b, r) : place(b, r) + A, :C
                        ]
            for back in (1, 2):
                if t - back >= 0:
                    for q in range(4):
                        value = product(phase, t, 2 - back, q)
                        if t + 1 < F and back == 1:
                            acc[t - 1, q] += value
                        else:
                            acc[t - back, q] = value

    for phase in range(3):
        for t in range(F):
            for dh, dw in SIDES:
                @pl.when(present(dh, dw))
                def _():
                    copy_to(phase, t, dh, dw).wait_send()


def local(cotangent, stored_first, stored_second, w_first, w_second, w_third):
    F, R, W, C = cotangent.shape
    sizes = (lax.axis_size("ha"), lax.axis_size("wa"), F, R, W, C)
    A, rows = W // NB, W * R // 2
    f32, bf16 = jnp.float32, jnp.bfloat16
    wbuf = pltpu.VMEM(w_first.shape, f32)
    block = pltpu.VMEM((F, R, W, C), f32)
    edge = -(-R // 8) * 8
    return pl.pallas_call(
        functools.partial(kernel, sizes),
        out_shape=pltpu.VMEM(cotangent.shape, jnp.float32),
        in_specs=[pl.BlockSpec(memory_space=pltpu.HBM)] * 6,
        out_specs=pl.BlockSpec(memory_space=pltpu.VMEM),
        scratch_shapes=[
            block, block, block,
            pltpu.VMEM((2, F, 2, rows, LANES), f32),
            wbuf, wbuf, wbuf,
            pltpu.VMEM((3, 3, 4, 2 * LANES, 3 * LANES), bf16),
            pltpu.VMEM((3, F, 2, rows, LANES), f32),
            pltpu.VMEM((F, 4, NB + 2, R // 2 * A, 2 * LANES), bf16),
            pltpu.VMEM((F, 4, rows, LANES), f32),
            pltpu.VMEM((3, F, 2, 3 * A, LANES), f32),
            pltpu.VMEM((3, F, 2, 3 * A, LANES), f32),
            pltpu.VMEM((3, F, 2, edge, LANES), f32),
            pltpu.VMEM((3, F, 2, edge, LANES), f32),
            pltpu.VMEM((3, F, 2, 2, edge, LANES), f32),
            pltpu.SemaphoreType.DMA((6,)),
            pltpu.SemaphoreType.DMA((3, F, 8)),
            pltpu.SemaphoreType.DMA((3, F, 8)),
        ],
        compiler_params=pltpu.CompilerParams(
            collective_id=0, has_side_effects=True,
            vmem_limit_bytes=67043328 - cotangent.size * 6,
        ),
    )(cotangent, stored_first, stored_second, w_first, w_second, w_third)


def solution(mesh):
    split_spec = P("clip", "ha", "wa", None)
    return jax.shard_map(
        local,
        mesh=mesh,
        in_specs=(split_spec, split_spec, split_spec, P(), P(), P()),
        out_specs=split_spec,
        check_vma=False,
    )
```

```python
import functools

import jax
import jax.numpy as jnp
from jax import lax
from jax.experimental import pallas as pl
from jax.experimental.pallas import tpu as pltpu
from jax.sharding import PartitionSpec as P

LANES = 128
NB = 4
SIDES = tuple((dh, dw) for dh in (-1, 0, 1) for dw in (-1, 0, 1) if (dh, dw) != (0, 0))
CORNERS = tuple(s for s in SIDES if s[0] and s[1])
COLS = ((0, -1), (0, 1))
ROWS = ((-1, 0), (1, 0))
ORDER = CORNERS + COLS + ROWS


def silu_slope(value):
    sigma = 1.0 / (1.0 + jnp.exp(-value))
    return sigma * (1.0 + value * (1.0 - sigma))


def split(value):
    high = value.astype(jnp.bfloat16)
    low = (value - high.astype(jnp.float32)).astype(jnp.bfloat16)
    return high, low


def kernel(
    sizes, cot, first, second, w1, w2, w3, out,
    vcot, sfirst, ssecond, slopes, wbuf0, wbuf1, wbuf2, wh, own, lhs, acc,
    zsend, zrecv, xsend, xrecv, crecv,
    local_sem, send_sem, recv_sem,
):
    nh, nw, F, R, W, C = sizes
    A, pairs = W // NB, R // 2
    rows = NB * pairs * A
    wbufs = (wbuf0, wbuf1, wbuf2)
    ih, iw = lax.axis_index("ha"), lax.axis_index("wa")

    def present(dh, dw):
        ok = ih >= 0
        if dh:
            ok = ok & ((ih > 0) if dh < 0 else (ih < nh - 1))
        if dw:
            ok = ok & ((iw > 0) if dw < 0 else (iw < nw - 1))
        return ok

    def one(flag):
        return jnp.where(flag, jnp.int32(1), jnp.int32(0))

    barrier = pltpu.get_barrier_semaphore()
    for dh, dw in SIDES:
        @pl.when(present(dh, dw))
        def _():
            pl.semaphore_signal(
                barrier, inc=1, device_id={"ha": ih + dh, "wa": iw + dw},
                device_id_type=pl.DeviceIdType.MESH,
            )

    loads = [
        pltpu.make_async_copy(cot, vcot, local_sem.at[0]),
        pltpu.make_async_copy(w3, wbuf0, local_sem.at[1]),
        pltpu.make_async_copy(second, ssecond, local_sem.at[4]),
        pltpu.make_async_copy(w2, wbuf1, local_sem.at[2]),
        pltpu.make_async_copy(first, sfirst, local_sem.at[5]),
        pltpu.make_async_copy(w1, wbuf2, local_sem.at[3]),
    ]
    for load in loads:
        load.start()

    def side(d):
        return (d + 1) // 2

    def landing(phase, t, dh, dw):
        if dh and dw:
            return crecv.at[phase, t, side(dh), side(dw)]
        if dw:
            return xrecv.at[phase, t, side(dw)]
        return zrecv.at[phase, t, side(dh)]

    def copy_to(phase, t, dh, dw):
        at = SIDES.index((dh, dw))
        source = xsend.at[phase, t, side(dw)] if dw else zsend.at[phase, t, side(dh)]
        return pltpu.make_async_remote_copy(
            src_ref=source,
            dst_ref=landing(phase, t, -dh, -dw),
            send_sem=send_sem.at[phase, t, at],
            recv_sem=recv_sem.at[phase, t, at],
            device_id={"ha": ih + dh, "wa": iw + dw},
            device_id_type=pl.DeviceIdType.MESH,
        )

    def send(phase, t):
        for dh, dw in ORDER:
            @pl.when(present(dh, dw))
            def _():
                copy_to(phase, t, dh, dw).start()

    def receive(phase, t):
        for dh, dw in ORDER:
            @pl.when(present(-dh, -dw))
            def _():
                copy_to(phase, t, dh, dw).wait_recv()

    for dh, dw in SIDES:
        @pl.when(jnp.logical_not(present(dh, dw)))
        def _():
            for phase in range(3):
                for t in range(F):
                    ref = landing(phase, t, dh, dw)
                    ref[...] = jnp.zeros(ref.shape, jnp.float32)

    lane = lax.broadcasted_iota(jnp.int32, (A, LANES), 1)
    line = lax.broadcasted_iota(jnp.int32, (A, LANES), 0)
    real = lane < C
    third = C // 3

    def wide(value):
        return jnp.concatenate(
            [value, jnp.zeros((value.shape[0], LANES - C), jnp.float32)], axis=1
        )

    def place(b, r):
        return (b * pairs + r // 2) * A

    def post(phase, t, tile):
        for r, to in ((0, 0), (R - 1, 1)):
            last = tile(r, NB - 1)
            for m in range(3):
                moved = pltpu.roll(last, LANES - third - third * m, axis=1)
                zsend[phase, t, to, m * A : (m + 1) * A, :] = jnp.where(real, tile(r, m), moved)
        for r in range(R):
            xsend[phase, t, 0, r : r + 1, :] = tile(r, 0)[0:1]
            xsend[phase, t, 1, r : r + 1, :] = tile(r, NB - 1)[A - 1 : A]

    def unpack(phase, t, to):
        packed = [zrecv[phase, t, to, m * A : (m + 1) * A, :] for m in range(3)]
        moved = [pltpu.roll(packed[m], third + third * m, axis=1) for m in range(3)]
        last = jnp.where(lane < third, moved[0], jnp.where(lane < 2 * third, moved[1], moved[2]))
        return [jnp.where(real, v, 0.0) for v in packed + [last]]

    xsend[...] = jnp.zeros_like(xsend)
    loads[0].wait()

    for t in reversed(range(F)):
        tiles = {}
        for r in range(R):
            for b in range(NB):
                tiles[r, b] = wide(vcot[t, r, pl.ds(b, A, stride=NB), :])
                own[0, t, r % 2, place(b, r) : place(b, r) + A, :] = tiles[r, b]
        post(0, t, lambda r, b: tiles[r, b])

    tall = 1 + one(ih > 0) + one(ih < nh - 1)
    broad = 1 + one(iw > 0) + one(iw < nw - 1)
    pl.semaphore_wait(barrier, tall * broad - 1)
    for t in reversed(range(F)):
        send(0, t)

    def prepare(phase):
        wbuf = wbufs[phase]

        @pl.loop(0, 3)
        def _(i):
            for k in range(3):
                g0, g1, g2 = (wide(jnp.transpose(wbuf[i, 2 - e, k])) for e in range(3))
                even, odd = (g0 + g2) * 0.5, g1 * 0.5
                for q, value in enumerate((g0, even + odd, even - odd, g2)):
                    high, low = split(value)
                    at = k * LANES
                    wh[phase, i, q, at : at + C, 0:LANES] = high
                    wh[phase, i, q, at : at + C, LANES:] = low
                    wh[phase, i, q, at + C : at + LANES, :] = jnp.zeros(
                        (LANES - C, 2 * LANES), jnp.bfloat16
                    )

    def slope_of(stored, at):
        @pl.loop(0, F)
        def _(t):
            for r in range(R):
                for b in range(NB):
                    slopes[at, t, r % 2, place(b, r) : place(b, r) + A, :] = wide(
                        silu_slope(stored[t, r, pl.ds(b, A, stride=NB), :])
                    )

    loads[1].wait()
    prepare(0)
    loads[2].wait()
    slope_of(ssecond, 0)
    loads[3].wait()
    prepare(1)
    loads[4].wait()
    slope_of(sfirst, 1)
    loads[5].wait()
    prepare(2)

    def arrange(phase, t):
        tiles = {}
        for r in range(-1, R + 1):
            if 0 <= r < R:
                for b in range(NB):
                    tiles[r, b] = own[phase, t, r % 2, place(b, r) : place(b, r) + A, :]
                left, right = (xrecv[phase, t, s, r : r + 1, :] for s in range(2))
            else:
                to = 0 if r < 0 else 1
                for b, value in enumerate(unpack(phase, t, to)):
                    tiles[r, b] = value
                near = R - 1 if r < 0 else 0
                left, right = (crecv[phase, t, to, s, near : near + 1, :] for s in range(2))
            tiles[r, -1] = jnp.where(line == 0, left, pltpu.roll(tiles[r, NB - 1], 1, axis=0))
            tiles[r, NB] = jnp.where(line == A - 1, right, pltpu.roll(tiles[r, 0], A - 1, axis=0))
        for p in range(pairs):
            for b in range(-1, NB + 1):
                d0, d1, d2, d3 = (tiles[2 * p - 1 + n, b] for n in range(4))
                for q, value in enumerate((d0 - d2, d1 + d2, d2 - d1, d1 - d3)):
                    high, low = split(value)
                    lhs[t, q, b + 1, p * A : (p + 1) * A, 0:LANES] = high
                    lhs[t, q, b + 1, p * A : (p + 1) * A, LANES:] = low

    def product(phase, t, i, q):
        a = jnp.concatenate(
            [lhs[t, q, 2 - k : 2 - k + NB].reshape(rows, 2 * LANES) for k in range(3)], axis=1
        )
        w = [wh[phase, i, q, k * LANES : (k + 1) * LANES] for k in range(3)]
        b = jnp.concatenate([w[0], w[0], w[1], w[1], w[2], w[2]], axis=0)
        value = jnp.dot(a, b, preferred_element_type=jnp.float32)
        return value[:, :LANES] + value[:, LANES:]

    for phase in range(3):
        for t in reversed(range(F)):
            receive(phase, t)
            arrange(phase, t)
            m = []
            for q in range(4):
                value = product(phase, t, 2, q)
                m.append(value if t == F - 1 else value + acc[t, q])
            done = (m[0] + m[1] + m[2], m[1] - m[2] - m[3])
            if phase < 2:
                done = [done[s] * slopes[phase, t, s] for s in range(2)]
                for s in range(2):
                    own[phase + 1, t, s] = done[s]
                post(phase + 1, t, lambda r, b: done[r % 2][place(b, r) : place(b, r) + A])
                send(phase + 1, t)
            else:
                for r in range(R):
                    for b in range(NB):
                        out[t, r, pl.ds(b, A, stride=NB), :] = done[r % 2][
                            place(b, r) : place(b, r) + A, :C
                        ]
            for back in (1, 2):
                if t - back >= 0:
                    for q in range(4):
                        value = product(phase, t, 2 - back, q)
                        if t + 1 < F and back == 1:
                            acc[t - 1, q] += value
                        else:
                            acc[t - back, q] = value

    for phase in range(3):
        for t in range(F):
            for dh, dw in SIDES:
                @pl.when(present(dh, dw))
                def _():
                    copy_to(phase, t, dh, dw).wait_send()


def local(cotangent, stored_first, stored_second, w_first, w_second, w_third):
    F, R, W, C = cotangent.shape
    sizes = (lax.axis_size("ha"), lax.axis_size("wa"), F, R, W, C)
    A, rows = W // NB, W * R // 2
    f32, bf16 = jnp.float32, jnp.bfloat16
    wbuf = pltpu.VMEM(w_first.shape, f32)
    block = pltpu.VMEM((F, R, W, C), f32)
    edge = -(-R // 8) * 8
    return pl.pallas_call(
        functools.partial(kernel, sizes),
        out_shape=pltpu.VMEM(cotangent.shape, jnp.float32),
        in_specs=[pl.BlockSpec(memory_space=pltpu.HBM)] * 6,
        out_specs=pl.BlockSpec(memory_space=pltpu.VMEM),
        scratch_shapes=[
            block, block, block,
            pltpu.VMEM((2, F, 2, rows, LANES), f32),
            wbuf, wbuf, wbuf,
            pltpu.VMEM((3, 3, 4, 3 * LANES, 2 * LANES), bf16),
            pltpu.VMEM((3, F, 2, rows, LANES), f32),
            pltpu.VMEM((F, 4, NB + 2, R // 2 * A, 2 * LANES), bf16),
            pltpu.VMEM((F, 4, rows, LANES), f32),
            pltpu.VMEM((3, F, 2, 3 * A, LANES), f32),
            pltpu.VMEM((3, F, 2, 3 * A, LANES), f32),
            pltpu.VMEM((3, F, 2, edge, LANES), f32),
            pltpu.VMEM((3, F, 2, edge, LANES), f32),
            pltpu.VMEM((3, F, 2, 2, edge, LANES), f32),
            pltpu.SemaphoreType.DMA((6,)),
            pltpu.SemaphoreType.DMA((3, F, 8)),
            pltpu.SemaphoreType.DMA((3, F, 8)),
        ],
        compiler_params=pltpu.CompilerParams(
            collective_id=0, has_side_effects=True,
            vmem_limit_bytes=67043328 - cotangent.size * 6,
        ),
    )(cotangent, stored_first, stored_second, w_first, w_second, w_third)


def solution(mesh):
    split_spec = P("clip", "ha", "wa", None)
    return jax.shard_map(
        local,
        mesh=mesh,
        in_specs=(split_spec, split_spec, split_spec, P(), P(), P()),
        out_specs=split_spec,
        check_vma=False,
    )
```

```python
import functools

import jax
import jax.numpy as jnp
from jax import lax
from jax.experimental import pallas as pl
from jax.experimental.pallas import tpu as pltpu
from jax.sharding import PartitionSpec as P

LANES = 128
EDGE = 8
NB = 4
SIDES = tuple((dh, dw) for dh in (-1, 0, 1) for dw in (-1, 0, 1) if (dh, dw) != (0, 0))
CORNERS = tuple(s for s in SIDES if s[0] and s[1])
COLS = ((0, -1), (0, 1))
ROWS = ((-1, 0), (1, 0))
ORDER = CORNERS + COLS + ROWS


def silu_slope(value):
    sigma = 1.0 / (1.0 + jnp.exp(-value))
    return sigma * (1.0 + value * (1.0 - sigma))


def split(value):
    high = value.astype(jnp.bfloat16)
    low = (value - high.astype(jnp.float32)).astype(jnp.bfloat16)
    return high, low


def kernel(
    sizes, cot, first, second, w1, w2, w3, out,
    vcot, sfirst, ssecond, slopes, wbuf0, wbuf1, wbuf2, wh, own, lhs, acc,
    zraw, xraw, craw, zsend, zrecv, xsend, xrecv, crecv, rawbytes, bytes_,
    local_sem, send_sem, recv_sem,
):
    nh, nw, F, R, W, C = sizes
    A, pairs = W // NB, R // 2
    rows = NB * pairs * A
    wbufs = (wbuf0, wbuf1, wbuf2)
    ih, iw = lax.axis_index("ha"), lax.axis_index("wa")

    def present(dh, dw):
        ok = ih >= 0
        if dh:
            ok = ok & ((ih > 0) if dh < 0 else (ih < nh - 1))
        if dw:
            ok = ok & ((iw > 0) if dw < 0 else (iw < nw - 1))
        return ok

    def one(flag):
        return jnp.where(flag, jnp.int32(1), jnp.int32(0))

    barrier = pltpu.get_barrier_semaphore()
    for dh, dw in SIDES:
        @pl.when(present(dh, dw))
        def _():
            pl.semaphore_signal(
                barrier, inc=1, device_id={"ha": ih + dh, "wa": iw + dw},
                device_id_type=pl.DeviceIdType.MESH,
            )

    loads = [
        pltpu.make_async_copy(cot, vcot, local_sem.at[0]),
        pltpu.make_async_copy(w3, wbuf0, local_sem.at[1]),
        pltpu.make_async_copy(second, ssecond, local_sem.at[4]),
        pltpu.make_async_copy(w2, wbuf1, local_sem.at[2]),
        pltpu.make_async_copy(first, sfirst, local_sem.at[5]),
        pltpu.make_async_copy(w1, wbuf2, local_sem.at[3]),
    ]
    for load in loads:
        load.start()

    def side(d):
        return (d + 1) // 2

    def landing(phase, t, dh, dw):
        if phase == 0:
            if dh and dw:
                return craw.at[t, side(dh), side(dw)]
            if dw:
                return xraw.at[t, side(dw)]
            return zraw.at[t, side(dh)]
        if dh and dw:
            return crecv.at[phase - 1, t, side(dh), side(dw)]
        if dw:
            return xrecv.at[phase - 1, t, side(dw)]
        return zrecv.at[phase - 1, t, side(dh)]

    def source(phase, t, dh, dw):
        if phase == 0:
            row = {-1: 0, 0: pl.ds(0, R), 1: R - 1}[dh]
            col = {-1: pl.ds(0, EDGE), 0: pl.ds(0, W), 1: pl.ds(W - EDGE, EDGE)}[dw]
            return cot.at[t, row, col, :]
        if dw:
            return xsend.at[phase - 1, t, side(dw)]
        return zsend.at[phase - 1, t, side(dh)]

    def arrival(phase, t):
        return recv_sem.at[phase % 2, t]

    def copy_to(phase, t, dh, dw):
        return pltpu.make_async_remote_copy(
            src_ref=source(phase, t, dh, dw),
            dst_ref=landing(phase, t, -dh, -dw),
            send_sem=send_sem.at[min(phase, 1)],
            recv_sem=arrival(phase, t),
            device_id={"ha": ih + dh, "wa": iw + dw},
            device_id_type=pl.DeviceIdType.MESH,
        )

    def send(phase, t):
        for dh, dw in ORDER:
            @pl.when(present(dh, dw))
            def _():
                copy_to(phase, t, dh, dw).start()

    def amount(phase, up, across):
        row = W // EDGE if phase == 0 else 3 * A // EDGE
        column = R if phase == 0 else xsend.shape[-2] // EDGE
        corner = 1 if phase == 0 else column
        return up * row + across * column + up * across * corner

    def by_neighbours(wait):
        for up in range(3):
            for across in range(3):
                if up + across:
                    @pl.when((tall == up + 1) & (broad == across + 1))
                    def _():
                        wait(up, across)

    def receive(phase, t):
        room = rawbytes if phase == 0 else bytes_

        def wait(up, across):
            part = room.at[0, pl.ds(0, amount(phase, up, across))]
            pltpu.make_async_copy(part, part, arrival(phase, t)).wait()

        by_neighbours(wait)

    tall = 1 + one(ih > 0) + one(ih < nh - 1)
    broad = 1 + one(iw > 0) + one(iw < nw - 1)
    pl.semaphore_wait(barrier, tall * broad - 1)
    for t in reversed(range(F)):
        send(0, t)

    for dh, dw in SIDES:
        @pl.when(jnp.logical_not(present(dh, dw)))
        def _():
            for phase in range(3):
                for t in range(F):
                    ref = landing(phase, t, dh, dw)
                    ref[...] = jnp.zeros(ref.shape, jnp.float32)

    lane = lax.broadcasted_iota(jnp.int32, (A, LANES), 1)
    line = lax.broadcasted_iota(jnp.int32, (A, LANES), 0)
    real = lane < C
    third = C // 3

    def wide(value):
        return jnp.concatenate(
            [value, jnp.zeros((value.shape[0], LANES - C), jnp.float32)], axis=1
        )

    def place(b, r):
        return (b * pairs + r // 2) * A

    def post(phase, t, tile):
        for r, to in ((0, 0), (R - 1, 1)):
            last = tile(r, NB - 1)
            for m in range(3):
                moved = pltpu.roll(last, LANES - third - third * m, axis=1)
                zsend[phase - 1, t, to, m * A : (m + 1) * A, :] = jnp.where(real, tile(r, m), moved)
        for r in range(R):
            xsend[phase - 1, t, 0, r : r + 1, :] = tile(r, 0)[0:1]
            xsend[phase - 1, t, 1, r : r + 1, :] = tile(r, NB - 1)[A - 1 : A]

    def unpack(phase, t, to):
        packed = [zrecv[phase - 1, t, to, m * A : (m + 1) * A, :] for m in range(3)]
        moved = [pltpu.roll(packed[m], third + third * m, axis=1) for m in range(3)]
        last = jnp.where(lane < third, moved[0], jnp.where(lane < 2 * third, moved[1], moved[2]))
        return [jnp.where(real, v, 0.0) for v in packed + [last]]

    xsend[...] = jnp.zeros_like(xsend)

    def prepare(phase):
        wbuf = wbufs[phase]

        @pl.loop(0, 3)
        def _(i):
            for k in range(3):
                g0, g1, g2 = (wide(jnp.transpose(wbuf[i, 2 - e, k])) for e in range(3))
                even, odd = (g0 + g2) * 0.5, g1 * 0.5
                for q, value in enumerate((g0, even + odd, even - odd, g2)):
                    high, low = split(value)
                    at = k * LANES
                    wh[phase, i, q, at : at + C, 0:LANES] = high
                    wh[phase, i, q, at : at + C, LANES:] = low
                    wh[phase, i, q, at + C : at + LANES, :] = jnp.zeros(
                        (LANES - C, 2 * LANES), jnp.bfloat16
                    )

    def slope_of(stored, at):
        @pl.loop(0, F)
        def _(t):
            for r in range(R):
                for b in range(NB):
                    slopes[at, t, r % 2, place(b, r) : place(b, r) + A, :] = wide(
                        silu_slope(stored[t, r, pl.ds(b, A, stride=NB), :])
                    )

    loads[0].wait()
    loads[1].wait()
    prepare(0)
    loads[2].wait()
    slope_of(ssecond, 0)
    loads[3].wait()
    prepare(1)
    loads[4].wait()
    slope_of(sfirst, 1)
    loads[5].wait()
    prepare(2)

    def arrange(phase, t):
        tiles = {}
        for r in range(-1, R + 1):
            to = 0 if r < 0 else 1
            near = R - 1 if r < 0 else 0
            if phase == 0:
                rows_ = vcot.at[t, r] if 0 <= r < R else zraw.at[t, to]
                for b in range(NB):
                    tiles[r, b] = wide(rows_[pl.ds(b, A, stride=NB), :])
                cells = xraw.at[:, :, r] if 0 <= r < R else craw.at[:, to]
                left, right = wide(cells[t, 0, EDGE - 1 :]), wide(cells[t, 1, 0:1])
            elif 0 <= r < R:
                for b in range(NB):
                    tiles[r, b] = own[phase - 1, t, r % 2, place(b, r) : place(b, r) + A, :]
                left, right = (xrecv[phase - 1, t, s, r : r + 1, :] for s in range(2))
            else:
                for b, value in enumerate(unpack(phase, t, to)):
                    tiles[r, b] = value
                left, right = (crecv[phase - 1, t, to, s, near : near + 1, :] for s in range(2))
            tiles[r, -1] = jnp.where(line == 0, left, pltpu.roll(tiles[r, NB - 1], 1, axis=0))
            tiles[r, NB] = jnp.where(line == A - 1, right, pltpu.roll(tiles[r, 0], A - 1, axis=0))
        for p in range(pairs):
            for b in range(-1, NB + 1):
                d0, d1, d2, d3 = (tiles[2 * p - 1 + n, b] for n in range(4))
                for q, value in enumerate((d0 - d2, d1 + d2, d2 - d1, d1 - d3)):
                    high, low = split(value)
                    lhs[t, q, b + 1, p * A : (p + 1) * A, 0:LANES] = high
                    lhs[t, q, b + 1, p * A : (p + 1) * A, LANES:] = low

    def product(phase, t, i, q):
        a = jnp.concatenate(
            [lhs[t, q, 2 - k : 2 - k + NB].reshape(rows, 2 * LANES) for k in range(3)], axis=1
        )
        w = [wh[phase, i, q, k * LANES : (k + 1) * LANES] for k in range(3)]
        b = jnp.concatenate([w[0], w[0], w[1], w[1], w[2], w[2]], axis=0)
        value = jnp.dot(a, b, preferred_element_type=jnp.float32)
        return value[:, :LANES] + value[:, LANES:]

    for phase in range(3):
        for t in reversed(range(F)):
            receive(phase, t)
            arrange(phase, t)
            m = []
            for q in range(4):
                value = product(phase, t, 2, q)
                m.append(value if t == F - 1 else value + acc[t, q])
            if 0 < t < F - 1:
                for q in range(4):
                    acc[t - 1, q] = product(phase, t + 1, 0, q)
            done = (m[0] + m[1] + m[2], m[1] - m[2] - m[3])
            if phase < 2:
                done = [done[s] * slopes[phase, t, s] for s in range(2)]
                for s in range(2):
                    own[phase, t, s] = done[s]
                post(phase + 1, t, lambda r, b: done[r % 2][place(b, r) : place(b, r) + A])
                send(phase + 1, t)
            else:
                for r in range(R):
                    for b in range(NB):
                        out[t, r, pl.ds(b, A, stride=NB), :] = done[r % 2][
                            place(b, r) : place(b, r) + A, :C
                        ]
            if t > 0:
                for q in range(4):
                    value = product(phase, t, 1, q)
                    acc[t - 1, q] = value if t == F - 1 else value + acc[t - 1, q]

    def sent(up, across):
        part = rawbytes.at[:, pl.ds(0, amount(0, up, across))]
        pltpu.make_async_copy(part, part, send_sem.at[0]).wait()
        part = bytes_.at[:, pl.ds(0, amount(1, up, across))]
        for _ in range(2):
            pltpu.make_async_copy(part, part, send_sem.at[1]).wait()

    by_neighbours(sent)


def local(cotangent, stored_first, stored_second, w_first, w_second, w_third):
    F, R, W, C = cotangent.shape
    sizes = (lax.axis_size("ha"), lax.axis_size("wa"), F, R, W, C)
    A, rows = W // NB, W * R // 2
    f32, bf16 = jnp.float32, jnp.bfloat16
    wbuf = pltpu.VMEM(w_first.shape, f32)
    block = pltpu.VMEM((F, R, W, C), f32)
    edge = -(-R // EDGE) * EDGE
    return pl.pallas_call(
        functools.partial(kernel, sizes),
        out_shape=pltpu.VMEM(cotangent.shape, jnp.float32),
        in_specs=[pl.BlockSpec(memory_space=pltpu.HBM)] * 6,
        out_specs=pl.BlockSpec(memory_space=pltpu.VMEM),
        scratch_shapes=[
            block, block, block,
            pltpu.VMEM((2, F, 2, rows, LANES), f32),
            wbuf, wbuf, wbuf,
            pltpu.VMEM((3, 3, 4, 3 * LANES, 2 * LANES), bf16),
            pltpu.VMEM((2, F, 2, rows, LANES), f32),
            pltpu.VMEM((F, 4, NB + 2, R // 2 * A, 2 * LANES), bf16),
            pltpu.VMEM((F, 4, rows, LANES), f32),
            pltpu.VMEM((F, 2, W, C), f32),
            pltpu.VMEM((F, 2, R, EDGE, C), f32),
            pltpu.VMEM((F, 2, 2, EDGE, C), f32),
            pltpu.VMEM((2, F, 2, 3 * A, LANES), f32),
            pltpu.VMEM((2, F, 2, 3 * A, LANES), f32),
            pltpu.VMEM((2, F, 2, edge, LANES), f32),
            pltpu.VMEM((2, F, 2, edge, LANES), f32),
            pltpu.VMEM((2, F, 2, 2, edge, LANES), f32),
            pltpu.VMEM((F, 2 * W // EDGE + 2 * R + 4, EDGE, C), f32),
            pltpu.VMEM((F, 6 * A // EDGE + 6 * edge // EDGE, EDGE, LANES), f32),
            pltpu.SemaphoreType.DMA((6,)),
            pltpu.SemaphoreType.DMA((2,)),
            pltpu.SemaphoreType.DMA((2, F)),
        ],
        compiler_params=pltpu.CompilerParams(
            collective_id=0, has_side_effects=True,
            vmem_limit_bytes=67043328 - cotangent.size * 6,
        ),
    )(cotangent, stored_first, stored_second, w_first, w_second, w_third)


def solution(mesh):
    split_spec = P("clip", "ha", "wa", None)
    return jax.shard_map(
        local,
        mesh=mesh,
        in_specs=(split_spec, split_spec, split_spec, P(), P(), P()),
        out_specs=split_spec,
        check_vma=False,
    )
```

```python
import functools

import jax
import jax.numpy as jnp
from jax import lax
from jax.experimental import pallas as pl
from jax.experimental.pallas import tpu as pltpu
from jax.sharding import PartitionSpec as P

LANES = 128
EDGE = 8
NB = 4
SIDES = tuple((dh, dw) for dh in (-1, 0, 1) for dw in (-1, 0, 1) if (dh, dw) != (0, 0))
CORNERS = tuple(s for s in SIDES if s[0] and s[1])
COLS = ((0, -1), (0, 1))
ROWS = ((-1, 0), (1, 0))
ORDER = CORNERS + COLS + ROWS


def silu_slope(value):
    sigma = 1.0 / (1.0 + jnp.exp(-value))
    return sigma * (1.0 + value * (1.0 - sigma))


def split(value):
    high = value.astype(jnp.bfloat16)
    low = (value - high.astype(jnp.float32)).astype(jnp.bfloat16)
    return high, low


def kernel(
    sizes, cot, first, second, w1, w2, w3, out,
    vcot, sfirst, ssecond, slopes, wbuf0, wbuf1, wbuf2, wh, own, lhs, acc,
    zsend, zrecv, xsend, xrecv, crecv, room,
    local_sem, send_sem, recv_sem,
):
    nh, nw, F, R, W, C = sizes
    A, pairs = W // NB, R // 2
    rows = NB * pairs * A
    wbufs = (wbuf0, wbuf1, wbuf2)
    ih, iw = lax.axis_index("ha"), lax.axis_index("wa")

    def present(dh, dw):
        ok = ih >= 0
        if dh:
            ok = ok & ((ih > 0) if dh < 0 else (ih < nh - 1))
        if dw:
            ok = ok & ((iw > 0) if dw < 0 else (iw < nw - 1))
        return ok

    def one(flag):
        return jnp.where(flag, jnp.int32(1), jnp.int32(0))

    barrier = pltpu.get_barrier_semaphore()
    for dh, dw in SIDES:
        @pl.when(present(dh, dw))
        def _():
            pl.semaphore_signal(
                barrier, inc=1, device_id={"ha": ih + dh, "wa": iw + dw},
                device_id_type=pl.DeviceIdType.MESH,
            )

    loads = [
        pltpu.make_async_copy(cot, vcot, local_sem.at[0]),
        pltpu.make_async_copy(w3, wbuf0, local_sem.at[1]),
        pltpu.make_async_copy(second, ssecond, local_sem.at[4]),
        pltpu.make_async_copy(w2, wbuf1, local_sem.at[2]),
        pltpu.make_async_copy(first, sfirst, local_sem.at[5]),
        pltpu.make_async_copy(w1, wbuf2, local_sem.at[3]),
    ]
    loads[0].start()

    def side(d):
        return (d + 1) // 2

    def landing(phase, t, dh, dw):
        if dh and dw:
            return crecv.at[phase, t, side(dh), side(dw)]
        if dw:
            return xrecv.at[phase, t, side(dw)]
        return zrecv.at[phase, t, side(dh)]

    def arrival(phase, t):
        return recv_sem.at[phase % 2, t]

    def copy_to(phase, t, dh, dw):
        return pltpu.make_async_remote_copy(
            src_ref=xsend.at[phase, t, side(dw)] if dw else zsend.at[phase, t, side(dh)],
            dst_ref=landing(phase, t, -dh, -dw),
            send_sem=send_sem.at[0],
            recv_sem=arrival(phase, t),
            device_id={"ha": ih + dh, "wa": iw + dw},
            device_id_type=pl.DeviceIdType.MESH,
        )

    def send(phase, t):
        for dh, dw in ORDER:
            @pl.when(present(dh, dw))
            def _():
                copy_to(phase, t, dh, dw).start()

    def amount(up, across):
        edge = xsend.shape[-2]
        return up * 3 * A + across * edge + up * across * edge

    def by_neighbours(wait):
        for up in range(3):
            for across in range(3):
                if up + across:
                    @pl.when((tall == up + 1) & (broad == across + 1))
                    def _():
                        wait(up, across)

    def receive(phase, t):
        def wait(up, across):
            part = room.at[0, 0, pl.ds(0, amount(up, across))]
            pltpu.make_async_copy(part, part, arrival(phase, t)).wait()

        by_neighbours(wait)

    tall = 1 + one(ih > 0) + one(ih < nh - 1)
    broad = 1 + one(iw > 0) + one(iw < nw - 1)

    for dh, dw in SIDES:
        @pl.when(jnp.logical_not(present(dh, dw)))
        def _():
            for phase in range(3):
                for t in range(F):
                    ref = landing(phase, t, dh, dw)
                    ref[...] = jnp.zeros(ref.shape, jnp.float32)

    lane = lax.broadcasted_iota(jnp.int32, (A, LANES), 1)
    line = lax.broadcasted_iota(jnp.int32, (A, LANES), 0)
    real = lane < C
    third = C // 3

    def wide(value):
        return jnp.concatenate(
            [value, jnp.zeros((value.shape[0], LANES - C), jnp.float32)], axis=1
        )

    def place(b, r):
        return (b * pairs + r // 2) * A

    def post(phase, t, tile):
        for r, to in ((0, 0), (R - 1, 1)):
            last = tile(r, NB - 1)
            for m in range(3):
                moved = pltpu.roll(last, LANES - third - third * m, axis=1)
                zsend[phase, t, to, m * A : (m + 1) * A, :] = jnp.where(real, tile(r, m), moved)
        for r in range(R):
            xsend[phase, t, 0, r : r + 1, :] = tile(r, 0)[0:1]
            xsend[phase, t, 1, r : r + 1, :] = tile(r, NB - 1)[A - 1 : A]

    def unpack(phase, t, to):
        packed = [zrecv[phase, t, to, m * A : (m + 1) * A, :] for m in range(3)]
        moved = [pltpu.roll(packed[m], third + third * m, axis=1) for m in range(3)]
        last = jnp.where(lane < third, moved[0], jnp.where(lane < 2 * third, moved[1], moved[2]))
        return [jnp.where(real, v, 0.0) for v in packed + [last]]

    xsend[...] = jnp.zeros_like(xsend)
    loads[0].wait()
    for load in loads[1:]:
        load.start()

    for t in reversed(range(F)):
        tiles = {}
        for r in range(R):
            for b in range(NB):
                tiles[r, b] = wide(vcot[t, r, pl.ds(b, A, stride=NB), :])
                own[0, t, r % 2, place(b, r) : place(b, r) + A, :] = tiles[r, b]
        post(0, t, lambda r, b: tiles[r, b])

    pl.semaphore_wait(barrier, tall * broad - 1)
    for t in reversed(range(F)):
        send(0, t)

    def prepare(phase):
        wbuf = wbufs[phase]

        @pl.loop(0, 3)
        def _(i):
            for k in range(3):
                g0, g1, g2 = (wide(jnp.transpose(wbuf[i, 2 - e, k])) for e in range(3))
                even, odd = (g0 + g2) * 0.5, g1 * 0.5
                for q, value in enumerate((g0, even + odd, even - odd, g2)):
                    high, low = split(value)
                    at = k * LANES
                    wh[phase, i, q, at : at + C, 0:LANES] = high
                    wh[phase, i, q, at : at + C, LANES:] = low
                    wh[phase, i, q, at + C : at + LANES, :] = jnp.zeros(
                        (LANES - C, 2 * LANES), jnp.bfloat16
                    )

    def slope_of(stored, at):
        @pl.loop(0, F)
        def _(t):
            for r in range(R):
                for b in range(NB):
                    slopes[at, t, r % 2, place(b, r) : place(b, r) + A, :] = wide(
                        silu_slope(stored[t, r, pl.ds(b, A, stride=NB), :])
                    )

    loads[1].wait()
    prepare(0)
    loads[2].wait()
    slope_of(ssecond, 0)
    loads[3].wait()
    prepare(1)
    loads[4].wait()
    slope_of(sfirst, 1)
    loads[5].wait()
    prepare(2)

    def arrange(phase, t):
        tiles = {}
        for r in range(-1, R + 1):
            to = 0 if r < 0 else 1
            near = R - 1 if r < 0 else 0
            if 0 <= r < R:
                for b in range(NB):
                    tiles[r, b] = own[phase, t, r % 2, place(b, r) : place(b, r) + A, :]
                left, right = (xrecv[phase, t, s, r : r + 1, :] for s in range(2))
            else:
                for b, value in enumerate(unpack(phase, t, to)):
                    tiles[r, b] = value
                left, right = (crecv[phase, t, to, s, near : near + 1, :] for s in range(2))
            tiles[r, -1] = jnp.where(line == 0, left, pltpu.roll(tiles[r, NB - 1], 1, axis=0))
            tiles[r, NB] = jnp.where(line == A - 1, right, pltpu.roll(tiles[r, 0], A - 1, axis=0))
        for p in range(pairs):
            for b in range(-1, NB + 1):
                d0, d1, d2, d3 = (tiles[2 * p - 1 + n, b] for n in range(4))
                for q, value in enumerate((d0 - d2, d1 + d2, d2 - d1, d1 - d3)):
                    high, low = split(value)
                    lhs[t, q, b + 1, p * A : (p + 1) * A, 0:LANES] = high
                    lhs[t, q, b + 1, p * A : (p + 1) * A, LANES:] = low

    def product(phase, t, q, taps):
        a, b = [], []
        for i in taps:
            for k in range(3):
                part = lhs[t + 2 - i, q, 2 - k : 2 - k + NB]
                a.append(part.reshape(rows, 2 * LANES))
                b += [wh[phase, i, q, k * LANES : (k + 1) * LANES]] * 2
        value = jnp.dot(
            jnp.concatenate(a, axis=1), jnp.concatenate(b, axis=0),
            preferred_element_type=jnp.float32,
        )
        return value[:, :LANES] + value[:, LANES:]

    ahead = (False, True, True)
    for phase in range(3):
        for t in reversed(range(F)):
            receive(phase, t)
            arrange(phase, t)
            older = range(max(0, t + 3 - F), 2)
            if ahead[phase] and older:
                m = [product(phase, t, q, (2,)) + acc[q] for q in range(4)]
            else:
                m = [product(phase, t, q, (*older, 2)) for q in range(4)]
            done = (m[0] + m[1] + m[2], m[1] - m[2] - m[3])
            if phase < 2:
                done = [done[s] * slopes[phase, t, s] for s in range(2)]
                for s in range(2):
                    own[phase + 1, t, s] = done[s]
                post(phase + 1, t, lambda r, b: done[r % 2][place(b, r) : place(b, r) + A])
                send(phase + 1, t)
            else:
                for r in range(R):
                    for b in range(NB):
                        out[t, r, pl.ds(b, A, stride=NB), :] = done[r % 2][
                            place(b, r) : place(b, r) + A, :C
                        ]
            if ahead[phase] and t > 0:
                for q in range(4):
                    acc[q] = product(phase, t - 1, q, range(max(0, t + 2 - F), 2))

    def sent(up, across):
        part = room.at[:, :, pl.ds(0, amount(up, across))]
        pltpu.make_async_copy(part, part, send_sem.at[0]).wait()

    by_neighbours(sent)


def local(cotangent, stored_first, stored_second, w_first, w_second, w_third):
    F, R, W, C = cotangent.shape
    sizes = (lax.axis_size("ha"), lax.axis_size("wa"), F, R, W, C)
    A, rows = W // NB, W * R // 2
    f32, bf16 = jnp.float32, jnp.bfloat16
    wbuf = pltpu.VMEM(w_first.shape, f32)
    block = pltpu.VMEM((F, R, W, C), f32)
    edge = -(-R // EDGE) * EDGE
    return pl.pallas_call(
        functools.partial(kernel, sizes),
        out_shape=pltpu.VMEM(cotangent.shape, jnp.float32),
        in_specs=[pl.BlockSpec(memory_space=pltpu.HBM)] * 6,
        out_specs=pl.BlockSpec(memory_space=pltpu.VMEM),
        scratch_shapes=[
            block, block, block,
            pltpu.VMEM((2, F, 2, rows, LANES), f32),
            wbuf, wbuf, wbuf,
            pltpu.VMEM((3, 3, 4, 3 * LANES, 2 * LANES), bf16),
            pltpu.VMEM((3, F, 2, rows, LANES), f32),
            pltpu.VMEM((F, 4, NB + 2, R // 2 * A, 2 * LANES), bf16),
            pltpu.VMEM((4, rows, LANES), f32),
            pltpu.VMEM((3, F, 2, 3 * A, LANES), f32),
            pltpu.VMEM((3, F, 2, 3 * A, LANES), f32),
            pltpu.VMEM((3, F, 2, edge, LANES), f32),
            pltpu.VMEM((3, F, 2, edge, LANES), f32),
            pltpu.VMEM((3, F, 2, 2, edge, LANES), f32),
            pltpu.VMEM((3, F, 6 * A + 6 * edge, LANES), f32),
            pltpu.SemaphoreType.DMA((6,)),
            pltpu.SemaphoreType.DMA((1,)),
            pltpu.SemaphoreType.DMA((2, F)),
        ],
        compiler_params=pltpu.CompilerParams(
            collective_id=0, has_side_effects=True,
            vmem_limit_bytes=67043328 - cotangent.size * 6,
        ),
    )(cotangent, stored_first, stored_second, w_first, w_second, w_third)


def solution(mesh):
    split_spec = P("clip", "ha", "wa", None)
    return jax.shard_map(
        local,
        mesh=mesh,
        in_specs=(split_spec, split_spec, split_spec, P(), P(), P()),
        out_specs=split_spec,
        check_vma=False,
    )
```

```python
import functools

import jax
import jax.numpy as jnp
from jax import lax
from jax.experimental import pallas as pl
from jax.experimental.pallas import tpu as pltpu
from jax.sharding import PartitionSpec as P

LANES = 128
EDGE = 8
NB = 4
SIDES = tuple((dh, dw) for dh in (-1, 0, 1) for dw in (-1, 0, 1) if (dh, dw) != (0, 0))
CORNERS = tuple(s for s in SIDES if s[0] and s[1])
COLS = ((0, -1), (0, 1))
ROWS = ((-1, 0), (1, 0))
ORDER = CORNERS + COLS + ROWS


def silu_slope(value):
    sigma = 1.0 / (1.0 + jnp.exp(-value))
    return sigma * (1.0 + value * (1.0 - sigma))


def split(value):
    high = value.astype(jnp.bfloat16)
    low = (value - high.astype(jnp.float32)).astype(jnp.bfloat16)
    return high, low


def kernel(
    sizes, cot, first, second, w1, w2, w3, out,
    vcot, sfirst, ssecond, wbuf0, wbuf1, wbuf2, wh, own, lhs, acc,
    zsend, zrecv, xsend, xrecv, crecv, room,
    local_sem, send_sem, recv_sem,
):
    nh, nw, F, R, W, C = sizes
    A, pairs = W // NB, R // 2
    rows = NB * pairs * A
    wbufs = (wbuf0, wbuf1, wbuf2)
    ih, iw = lax.axis_index("ha"), lax.axis_index("wa")

    def present(dh, dw):
        ok = ih >= 0
        if dh:
            ok = ok & ((ih > 0) if dh < 0 else (ih < nh - 1))
        if dw:
            ok = ok & ((iw > 0) if dw < 0 else (iw < nw - 1))
        return ok

    def one(flag):
        return jnp.where(flag, jnp.int32(1), jnp.int32(0))

    barrier = pltpu.get_barrier_semaphore()
    for dh, dw in SIDES:
        @pl.when(present(dh, dw))
        def _():
            pl.semaphore_signal(
                barrier, inc=1, device_id={"ha": ih + dh, "wa": iw + dw},
                device_id_type=pl.DeviceIdType.MESH,
            )

    loads = [
        pltpu.make_async_copy(
            cot.at[:, pl.ds(1, R - 2), pl.ds(EDGE, W - 2 * EDGE)],
            vcot.at[:, pl.ds(1, R - 2), pl.ds(EDGE, W - 2 * EDGE)], local_sem.at[0],
        ),
        pltpu.make_async_copy(w3, wbuf0, local_sem.at[1]),
        pltpu.make_async_copy(second, ssecond, local_sem.at[4]),
        pltpu.make_async_copy(w2, wbuf1, local_sem.at[2]),
        pltpu.make_async_copy(first, sfirst, local_sem.at[5]),
        pltpu.make_async_copy(w1, wbuf2, local_sem.at[3]),
    ]
    rim = [
        pltpu.make_async_copy(cot.at[:, r, c], vcot.at[:, r, c], local_sem.at[6 + n])
        for n, (r, c) in enumerate((
            (0, pl.ds(0, W)), (R - 1, pl.ds(0, W)),
            (pl.ds(1, R - 2), pl.ds(0, EDGE)), (pl.ds(1, R - 2), pl.ds(W - EDGE, EDGE)),
        ))
    ]
    for load in rim:
        load.start()

    def side(d):
        return (d + 1) // 2

    def landing(phase, t, dh, dw):
        if dh and dw:
            return crecv.at[phase, t, side(dh), side(dw)]
        if dw:
            return xrecv.at[phase, t, side(dw)]
        return zrecv.at[phase, t, side(dh)]

    def arrival(phase, t):
        return recv_sem.at[phase % 2, t]

    def copy_to(phase, t, dh, dw):
        return pltpu.make_async_remote_copy(
            src_ref=xsend.at[phase, t, side(dw)] if dw else zsend.at[phase, t, side(dh)],
            dst_ref=landing(phase, t, -dh, -dw),
            send_sem=send_sem.at[0],
            recv_sem=arrival(phase, t),
            device_id={"ha": ih + dh, "wa": iw + dw},
            device_id_type=pl.DeviceIdType.MESH,
        )

    def send(phase, t):
        for dh, dw in ORDER:
            @pl.when(present(dh, dw))
            def _():
                copy_to(phase, t, dh, dw).start()

    def amount(up, across):
        edge = xsend.shape[-2]
        return up * 3 * A + across * edge + up * across * edge

    def by_neighbours(wait):
        for up in range(3):
            for across in range(3):
                if up + across:
                    @pl.when((tall == up + 1) & (broad == across + 1))
                    def _():
                        wait(up, across)

    def receive(phase, t):
        def wait(up, across):
            part = room.at[0, 0, pl.ds(0, amount(up, across))]
            pltpu.make_async_copy(part, part, arrival(phase, t)).wait()

        by_neighbours(wait)

    tall = 1 + one(ih > 0) + one(ih < nh - 1)
    broad = 1 + one(iw > 0) + one(iw < nw - 1)

    for dh, dw in SIDES:
        @pl.when(jnp.logical_not(present(dh, dw)))
        def _():
            for phase in range(3):
                for t in range(F):
                    ref = landing(phase, t, dh, dw)
                    ref[...] = jnp.zeros(ref.shape, jnp.float32)

    lane = lax.broadcasted_iota(jnp.int32, (A, LANES), 1)
    line = lax.broadcasted_iota(jnp.int32, (A, LANES), 0)
    real = lane < C
    third = C // 3

    def wide(value):
        return jnp.concatenate(
            [value, jnp.zeros((value.shape[0], LANES - C), jnp.float32)], axis=1
        )

    def place(b, r):
        return (b * pairs + r // 2) * A

    def post(phase, t, tile, cell=None):
        if cell is None:
            def cell(r, w):
                a = w // NB
                return tile(r, w % NB)[a : a + 1]

        for r, to in ((0, 0), (R - 1, 1)):
            last = tile(r, NB - 1)
            for m in range(3):
                moved = pltpu.roll(last, LANES - third - third * m, axis=1)
                zsend[phase, t, to, m * A : (m + 1) * A, :] = jnp.where(real, tile(r, m), moved)
        for r in range(R):
            xsend[phase, t, 0, r : r + 1, :] = cell(r, 0)
            xsend[phase, t, 1, r : r + 1, :] = cell(r, W - 1)

    def unpack(phase, t, to):
        packed = [zrecv[phase, t, to, m * A : (m + 1) * A, :] for m in range(3)]
        moved = [pltpu.roll(packed[m], third + third * m, axis=1) for m in range(3)]
        last = jnp.where(lane < third, moved[0], jnp.where(lane < 2 * third, moved[1], moved[2]))
        return [jnp.where(real, v, 0.0) for v in packed + [last]]

    xsend[...] = jnp.zeros_like(xsend)
    for load in rim:
        load.wait()
    for load in loads:
        load.start()

    def given(t, r, b):
        return wide(vcot[t, r, pl.ds(b, A, stride=NB), :])

    def given_cell(t, r, w):
        return wide(vcot[t, r, w : w + 1, :])

    post(0, F - 1, functools.partial(given, F - 1), functools.partial(given_cell, F - 1))
    pl.semaphore_wait(barrier, tall * broad - 1)
    send(0, F - 1)
    for t in reversed(range(F - 1)):
        post(0, t, functools.partial(given, t), functools.partial(given_cell, t))
        send(0, t)

    def prepare(phase, i):
        for k in range(3):
            g0, g1, g2 = (wide(jnp.transpose(wbufs[phase][i, 2 - e, k])) for e in range(3))
            even, odd = (g0 + g2) * 0.5, g1 * 0.5
            for q, value in enumerate((g0, even + odd, even - odd, g2)):
                high, low = split(value)
                at = k * LANES
                wh[phase, i, q, at : at + C, 0:LANES] = high
                wh[phase, i, q, at : at + C, LANES:] = low
                wh[phase, i, q, at + C : at + LANES, :] = jnp.zeros(
                    (LANES - C, 2 * LANES), jnp.bfloat16
                )

    def slope_of(stored, t, s):
        order = [(b, r) for b in range(NB) for r in range(s, R, 2)]
        values = [wide(stored[t, r, pl.ds(b, A, stride=NB), :]) for b, r in order]
        return jnp.concatenate([silu_slope(value) for value in values], axis=0)

    loads[0].wait()
    loads[1].wait()

    @pl.loop(0, 3)
    def _(i):
        prepare(0, i)

    for load in loads[2:]:
        load.wait()

    def arrange(phase, t):
        tiles = {}
        for r in range(-1, R + 1):
            to = 0 if r < 0 else 1
            near = R - 1 if r < 0 else 0
            if 0 <= r < R:
                for b in range(NB):
                    at = place(b, r)
                    tiles[r, b] = own[phase - 1, t, r % 2, at : at + A, :] if phase else given(t, r, b)
                left, right = (xrecv[phase, t, s, r : r + 1, :] for s in range(2))
            else:
                for b, value in enumerate(unpack(phase, t, to)):
                    tiles[r, b] = value
                left, right = (crecv[phase, t, to, s, near : near + 1, :] for s in range(2))
            tiles[r, -1] = jnp.where(line == 0, left, pltpu.roll(tiles[r, NB - 1], 1, axis=0))
            tiles[r, NB] = jnp.where(line == A - 1, right, pltpu.roll(tiles[r, 0], A - 1, axis=0))
        for p in range(pairs):
            for b in range(-1, NB + 1):
                d0, d1, d2, d3 = (tiles[2 * p - 1 + n, b] for n in range(4))
                for q, value in enumerate((d0 - d2, d1 + d2, d2 - d1, d1 - d3)):
                    high, low = split(value)
                    lhs[t, q, b + 1, p * A : (p + 1) * A, 0:LANES] = high
                    lhs[t, q, b + 1, p * A : (p + 1) * A, LANES:] = low

    def product(phase, t, q, taps):
        a, b = [], []
        for i in taps:
            for k in range(3):
                part = lhs[t + 2 - i, q, 2 - k : 2 - k + NB]
                a.append(part.reshape(rows, 2 * LANES))
                b += [wh[phase, i, q, k * LANES : (k + 1) * LANES]] * 2
        value = jnp.dot(
            jnp.concatenate(a, axis=1), jnp.concatenate(b, axis=0),
            preferred_element_type=jnp.float32,
        )
        return value[:, :LANES] + value[:, LANES:]

    def ahead(phase, t):
        older = range(max(0, t + 3 - F), 2)
        return tuple(i for i in older if phase == 2 or (phase == 1 and (t == 2 or (t == 1 and i == 0))))

    for phase in range(3):
        for t in reversed(range(F)):
            receive(phase, t)
            arrange(phase, t)
            if phase < 2 and t < 3:
                prepare(phase + 1, t)
            early = ahead(phase, t)
            late = [i for i in range(max(0, t + 3 - F), 3) if i not in early]
            m = [product(phase, t, q, late) for q in range(4)]
            if early:
                m = [m[q] + acc[q] for q in range(4)]
            done = (m[0] + m[1] + m[2], m[1] - m[2] - m[3])
            if phase < 2:
                stored = (ssecond, sfirst)[phase]
                done = [done[s] * slope_of(stored, t, s) for s in range(2)]
                for s in range(2):
                    own[phase, t, s] = done[s]
                post(phase + 1, t, lambda r, b: done[r % 2][place(b, r) : place(b, r) + A])
                send(phase + 1, t)
            else:
                for r in range(R):
                    for b in range(NB):
                        out[t, r, pl.ds(b, A, stride=NB), :] = done[r % 2][
                            place(b, r) : place(b, r) + A, :C
                        ]
            if t > 0 and ahead(phase, t - 1):
                for q in range(4):
                    acc[q] = product(phase, t - 1, q, ahead(phase, t - 1))

    def sent(up, across):
        part = room.at[:, :, pl.ds(0, amount(up, across))]
        pltpu.make_async_copy(part, part, send_sem.at[0]).wait()

    by_neighbours(sent)


def local(cotangent, stored_first, stored_second, w_first, w_second, w_third):
    F, R, W, C = cotangent.shape
    sizes = (lax.axis_size("ha"), lax.axis_size("wa"), F, R, W, C)
    A, rows = W // NB, W * R // 2
    f32, bf16 = jnp.float32, jnp.bfloat16
    wbuf = pltpu.VMEM(w_first.shape, f32)
    block = pltpu.VMEM((F, R, W, C), f32)
    edge = -(-R // EDGE) * EDGE
    return pl.pallas_call(
        functools.partial(kernel, sizes),
        out_shape=pltpu.VMEM(cotangent.shape, jnp.float32),
        in_specs=[pl.BlockSpec(memory_space=pltpu.HBM)] * 6,
        out_specs=pl.BlockSpec(memory_space=pltpu.VMEM),
        scratch_shapes=[
            block, block, block,
            wbuf, wbuf, wbuf,
            pltpu.VMEM((3, 3, 4, 3 * LANES, 2 * LANES), bf16),
            pltpu.VMEM((2, F, 2, rows, LANES), f32),
            pltpu.VMEM((F, 4, NB + 2, R // 2 * A, 2 * LANES), bf16),
            pltpu.VMEM((4, rows, LANES), f32),
            pltpu.VMEM((3, F, 2, 3 * A, LANES), f32),
            pltpu.VMEM((3, F, 2, 3 * A, LANES), f32),
            pltpu.VMEM((3, F, 2, edge, LANES), f32),
            pltpu.VMEM((3, F, 2, edge, LANES), f32),
            pltpu.VMEM((3, F, 2, 2, edge, LANES), f32),
            pltpu.VMEM((3, F, 6 * A + 6 * edge, LANES), f32),
            pltpu.SemaphoreType.DMA((10,)),
            pltpu.SemaphoreType.DMA((1,)),
            pltpu.SemaphoreType.DMA((2, F)),
        ],
        compiler_params=pltpu.CompilerParams(
            collective_id=0, has_side_effects=True,
            vmem_limit_bytes=67043328 - cotangent.size * 6,
        ),
    )(cotangent, stored_first, stored_second, w_first, w_second, w_third)


def solution(mesh):
    split_spec = P("clip", "ha", "wa", None)
    return jax.shard_map(
        local,
        mesh=mesh,
        in_specs=(split_spec, split_spec, split_spec, P(), P(), P()),
        out_specs=split_spec,
        check_vma=False,
    )
```

```python
import functools

import jax
import jax.numpy as jnp
from jax import lax
from jax.experimental import pallas as pl
from jax.experimental.pallas import tpu as pltpu
from jax.sharding import PartitionSpec as P

LANES = 128
EDGE = 8
NB = 4
SIDES = tuple((dh, dw) for dh in (-1, 0, 1) for dw in (-1, 0, 1) if (dh, dw) != (0, 0))
CORNERS = tuple(s for s in SIDES if s[0] and s[1])
COLS = ((0, -1), (0, 1))
ROWS = ((-1, 0), (1, 0))
ORDER = CORNERS + COLS + ROWS


def silu_slope(value):
    sigma = 1.0 / (1.0 + jnp.exp(-value))
    return sigma * (1.0 + value * (1.0 - sigma))


def split(value):
    high = value.astype(jnp.bfloat16)
    low = (value - high.astype(jnp.float32)).astype(jnp.bfloat16)
    return high, low


def kernel(
    sizes, cot, first, second, w1, w2, w3, out,
    vcot, sfirst, ssecond, wbuf0, wbuf1, wbuf2, wh, own, lhs, acc, slopes,
    zsend, zrecv, xsend, xrecv, crecv, room,
    local_sem, send_sem, recv_sem,
):
    nh, nw, F, R, W, C = sizes
    A, pairs = W // NB, R // 2
    rows = NB * pairs * A
    wbufs = (wbuf0, wbuf1, wbuf2)
    ih, iw = lax.axis_index("ha"), lax.axis_index("wa")

    def present(dh, dw):
        ok = ih >= 0
        if dh:
            ok = ok & ((ih > 0) if dh < 0 else (ih < nh - 1))
        if dw:
            ok = ok & ((iw > 0) if dw < 0 else (iw < nw - 1))
        return ok

    def one(flag):
        return jnp.where(flag, jnp.int32(1), jnp.int32(0))

    barrier = pltpu.get_barrier_semaphore()
    for dh, dw in SIDES:
        @pl.when(present(dh, dw))
        def _():
            pl.semaphore_signal(
                barrier, inc=1, device_id={"ha": ih + dh, "wa": iw + dw},
                device_id_type=pl.DeviceIdType.MESH,
            )

    loads = [
        pltpu.make_async_copy(
            cot.at[:, pl.ds(1, R - 2), pl.ds(EDGE, W - 2 * EDGE)],
            vcot.at[:, pl.ds(1, R - 2), pl.ds(EDGE, W - 2 * EDGE)], local_sem.at[0],
        ),
        pltpu.make_async_copy(w3, wbuf0, local_sem.at[1]),
        pltpu.make_async_copy(second, ssecond, local_sem.at[4]),
        pltpu.make_async_copy(w2, wbuf1, local_sem.at[2]),
        pltpu.make_async_copy(first, sfirst, local_sem.at[5]),
        pltpu.make_async_copy(w1, wbuf2, local_sem.at[3]),
    ]
    rim = [
        pltpu.make_async_copy(cot.at[:, r, c], vcot.at[:, r, c], local_sem.at[6 + n])
        for n, (r, c) in enumerate((
            (0, pl.ds(0, W)), (R - 1, pl.ds(0, W)),
            (pl.ds(1, R - 2), pl.ds(0, EDGE)), (pl.ds(1, R - 2), pl.ds(W - EDGE, EDGE)),
        ))
    ]
    for load in rim:
        load.start()

    def side(d):
        return (d + 1) // 2

    def landing(phase, t, dh, dw):
        if dh and dw:
            return crecv.at[phase, t, side(dh), side(dw)]
        if dw:
            return xrecv.at[phase, t, side(dw)]
        return zrecv.at[phase, t, side(dh)]

    def arrival(phase, t):
        return recv_sem.at[phase % 2, t]

    def copy_to(phase, t, dh, dw):
        return pltpu.make_async_remote_copy(
            src_ref=xsend.at[phase, t, side(dw)] if dw else zsend.at[phase, t, side(dh)],
            dst_ref=landing(phase, t, -dh, -dw),
            send_sem=send_sem.at[0],
            recv_sem=arrival(phase, t),
            device_id={"ha": ih + dh, "wa": iw + dw},
            device_id_type=pl.DeviceIdType.MESH,
        )

    def send(phase, t):
        for dh, dw in ORDER:
            @pl.when(present(dh, dw))
            def _():
                copy_to(phase, t, dh, dw).start()

    def amount(up, across):
        edge = xsend.shape[-2]
        return up * 3 * A + across * edge + up * across * edge

    def by_neighbours(wait):
        for up in range(3):
            for across in range(3):
                if up + across:
                    @pl.when((tall == up + 1) & (broad == across + 1))
                    def _():
                        wait(up, across)

    def receive(phase, t):
        def wait(up, across):
            part = room.at[0, 0, pl.ds(0, amount(up, across))]
            pltpu.make_async_copy(part, part, arrival(phase, t)).wait()

        by_neighbours(wait)

    tall = 1 + one(ih > 0) + one(ih < nh - 1)
    broad = 1 + one(iw > 0) + one(iw < nw - 1)

    for dh, dw in SIDES:
        @pl.when(jnp.logical_not(present(dh, dw)))
        def _():
            for phase in range(3):
                for t in range(F):
                    ref = landing(phase, t, dh, dw)
                    ref[...] = jnp.zeros(ref.shape, jnp.float32)

    lane = lax.broadcasted_iota(jnp.int32, (A, LANES), 1)
    line = lax.broadcasted_iota(jnp.int32, (A, LANES), 0)
    real = lane < C
    third = C // 3

    def wide(value):
        return jnp.concatenate(
            [value, jnp.zeros((value.shape[0], LANES - C), jnp.float32)], axis=1
        )

    def place(b, r):
        return (b * pairs + r // 2) * A

    def post(phase, t, tile, cell=None):
        if cell is None:
            def cell(r, w):
                a = w // NB
                return tile(r, w % NB)[a : a + 1]

        for r, to in ((0, 0), (R - 1, 1)):
            last = tile(r, NB - 1)
            for m in range(3):
                moved = pltpu.roll(last, LANES - third - third * m, axis=1)
                zsend[phase, t, to, m * A : (m + 1) * A, :] = jnp.where(real, tile(r, m), moved)
        for r in range(R):
            xsend[phase, t, 0, r : r + 1, :] = cell(r, 0)
            xsend[phase, t, 1, r : r + 1, :] = cell(r, W - 1)

    def unpack(phase, t, to):
        packed = [zrecv[phase, t, to, m * A : (m + 1) * A, :] for m in range(3)]
        moved = [pltpu.roll(packed[m], third + third * m, axis=1) for m in range(3)]
        last = jnp.where(lane < third, moved[0], jnp.where(lane < 2 * third, moved[1], moved[2]))
        return [jnp.where(real, v, 0.0) for v in packed + [last]]

    xsend[...] = jnp.zeros_like(xsend)
    for load in rim:
        load.wait()
    for load in loads:
        load.start()

    def given(t, r, b):
        return wide(vcot[t, r, pl.ds(b, A, stride=NB), :])

    def given_cell(t, r, w):
        return wide(vcot[t, r, w : w + 1, :])

    post(0, F - 1, functools.partial(given, F - 1), functools.partial(given_cell, F - 1))
    pl.semaphore_wait(barrier, tall * broad - 1)
    send(0, F - 1)
    for t in reversed(range(F - 1)):
        post(0, t, functools.partial(given, t), functools.partial(given_cell, t))
        send(0, t)

    def prepare(phase, i):
        for k in range(3):
            g0, g1, g2 = (wide(jnp.transpose(wbufs[phase][i, 2 - e, k])) for e in range(3))
            even, odd = (g0 + g2) * 0.5, g1 * 0.5
            for q, value in enumerate((g0, even + odd, even - odd, g2)):
                high, low = split(value)
                at = k * LANES
                wh[phase, i, q, at : at + C, 0:LANES] = high
                wh[phase, i, q, at : at + C, LANES:] = low
                wh[phase, i, q, at + C : at + LANES, :] = jnp.zeros(
                    (LANES - C, 2 * LANES), jnp.bfloat16
                )

    def slope_of(stored, t, s):
        order = [(b, r) for b in range(NB) for r in range(s, R, 2)]
        values = [wide(stored[t, r, pl.ds(b, A, stride=NB), :]) for b, r in order]
        return jnp.concatenate([silu_slope(value) for value in values], axis=0)

    loads[0].wait()
    loads[1].wait()

    @pl.loop(0, 3)
    def _(i):
        prepare(0, i)

    for load in loads[2:]:
        load.wait()
    for s in range(2):
        slopes[F - 1, s] = slope_of(ssecond, F - 1, s)

    def arrange(phase, t):
        tiles = {}
        for r in range(-1, R + 1):
            to = 0 if r < 0 else 1
            near = R - 1 if r < 0 else 0
            if 0 <= r < R:
                for b in range(NB):
                    at = place(b, r)
                    tiles[r, b] = own[phase - 1, t, r % 2, at : at + A, :] if phase else given(t, r, b)
                left, right = (xrecv[phase, t, s, r : r + 1, :] for s in range(2))
            else:
                for b, value in enumerate(unpack(phase, t, to)):
                    tiles[r, b] = value
                left, right = (crecv[phase, t, to, s, near : near + 1, :] for s in range(2))
            tiles[r, -1] = jnp.where(line == 0, left, pltpu.roll(tiles[r, NB - 1], 1, axis=0))
            tiles[r, NB] = jnp.where(line == A - 1, right, pltpu.roll(tiles[r, 0], A - 1, axis=0))
        for p in range(pairs):
            for b in range(-1, NB + 1):
                d0, d1, d2, d3 = (tiles[2 * p - 1 + n, b] for n in range(4))
                for q, value in enumerate((d0 - d2, d1 + d2, d2 - d1, d1 - d3)):
                    high, low = split(value)
                    lhs[t, q, b + 1, p * A : (p + 1) * A, 0:LANES] = high
                    lhs[t, q, b + 1, p * A : (p + 1) * A, LANES:] = low

    def product(phase, t, q, taps):
        a, b = [], []
        for i in taps:
            for k in range(3):
                part = lhs[t + 2 - i, q, 2 - k : 2 - k + NB]
                a.append(part.reshape(rows, 2 * LANES))
                b += [wh[phase, i, q, k * LANES : (k + 1) * LANES]] * 2
        value = jnp.dot(
            jnp.concatenate(a, axis=1), jnp.concatenate(b, axis=0),
            preferred_element_type=jnp.float32,
        )
        return value[:, :LANES] + value[:, LANES:]

    def ahead(phase, t):
        older = range(max(0, t + 3 - F), 2)
        return tuple(i for i in older if phase == 2 or (phase == 1 and (t == 2 or (t == 1 and i == 0))))

    for phase in range(3):
        for t in reversed(range(F)):
            receive(phase, t)
            arrange(phase, t)
            if phase < 2 and t < 3:
                prepare(phase + 1, t)
            early = ahead(phase, t)
            late = [i for i in range(max(0, t + 3 - F), 3) if i not in early]
            m = [product(phase, t, q, late) for q in range(4)]
            if early:
                m = [m[q] + acc[q] for q in range(4)]
            done = (m[0] + m[1] + m[2], m[1] - m[2] - m[3])
            if phase < 2:
                stored = (ssecond, sfirst)[phase]
                done = [done[s] * slopes[t, s] for s in range(2)]
                for s in range(2):
                    own[phase, t, s] = done[s]
                post(phase + 1, t, lambda r, b: done[r % 2][place(b, r) : place(b, r) + A])
                send(phase + 1, t)
            else:
                for r in range(R):
                    for b in range(NB):
                        out[t, r, pl.ds(b, A, stride=NB), :] = done[r % 2][
                            place(b, r) : place(b, r) + A, :C
                        ]
            if phase < 2:
                stored, n = (ssecond, t - 1) if t > 0 and phase == 0 else (sfirst, (t - 1) % F)
                if phase == 0 or t > 0:
                    for s in range(2):
                        slopes[n, s] = slope_of(stored, n, s)
            if t > 0 and ahead(phase, t - 1):
                for q in range(4):
                    acc[q] = product(phase, t - 1, q, ahead(phase, t - 1))

    def sent(up, across):
        part = room.at[:, :, pl.ds(0, amount(up, across))]
        pltpu.make_async_copy(part, part, send_sem.at[0]).wait()

    by_neighbours(sent)


def local(cotangent, stored_first, stored_second, w_first, w_second, w_third):
    F, R, W, C = cotangent.shape
    sizes = (lax.axis_size("ha"), lax.axis_size("wa"), F, R, W, C)
    A, rows = W // NB, W * R // 2
    f32, bf16 = jnp.float32, jnp.bfloat16
    wbuf = pltpu.VMEM(w_first.shape, f32)
    block = pltpu.VMEM((F, R, W, C), f32)
    edge = -(-R // EDGE) * EDGE
    return pl.pallas_call(
        functools.partial(kernel, sizes),
        out_shape=pltpu.VMEM(cotangent.shape, jnp.float32),
        in_specs=[pl.BlockSpec(memory_space=pltpu.HBM)] * 6,
        out_specs=pl.BlockSpec(memory_space=pltpu.VMEM),
        scratch_shapes=[
            block, block, block,
            wbuf, wbuf, wbuf,
            pltpu.VMEM((3, 3, 4, 3 * LANES, 2 * LANES), bf16),
            pltpu.VMEM((2, F, 2, rows, LANES), f32),
            pltpu.VMEM((F, 4, NB + 2, R // 2 * A, 2 * LANES), bf16),
            pltpu.VMEM((4, rows, LANES), f32),
            pltpu.VMEM((F, 2, rows, LANES), f32),
            pltpu.VMEM((3, F, 2, 3 * A, LANES), f32),
            pltpu.VMEM((3, F, 2, 3 * A, LANES), f32),
            pltpu.VMEM((3, F, 2, edge, LANES), f32),
            pltpu.VMEM((3, F, 2, edge, LANES), f32),
            pltpu.VMEM((3, F, 2, 2, edge, LANES), f32),
            pltpu.VMEM((3, F, 6 * A + 6 * edge, LANES), f32),
            pltpu.SemaphoreType.DMA((10,)),
            pltpu.SemaphoreType.DMA((1,)),
            pltpu.SemaphoreType.DMA((2, F)),
        ],
        compiler_params=pltpu.CompilerParams(
            collective_id=0, has_side_effects=True,
            vmem_limit_bytes=67043328 - cotangent.size * 6,
        ),
    )(cotangent, stored_first, stored_second, w_first, w_second, w_third)


def solution(mesh):
    split_spec = P("clip", "ha", "wa", None)
    return jax.shard_map(
        local,
        mesh=mesh,
        in_specs=(split_spec, split_spec, split_spec, P(), P(), P()),
        out_specs=split_spec,
        check_vma=False,
    )
```
